256 devices in a mesh: groups: 4 (over x, y), seq: 32 (over z), pd: 2 (over core).
Axes of the slice: x: 2, y: 2, z: 32, core: 2. Of those that a mesh axis runs over, the one named last changes fastest.
The devices are a block of a 4x8x32 slice.
Arguments:
- streams: bfloat16 [32768, 4, 7168], P(('groups', 'seq'), None, 'pd'), parts along dimension 0, may hold values from -6 to 6
- mix_first: bfloat16 [4, 7168, 24], P(None, 'pd'), may hold values from -0.03125 to 0.03125
- first_layer_bias: float32 [24], replicated, may hold values from -3 to 3
- pre_second: bfloat16 [4, 7168, 4], P(None, 'pd'), may hold values from -0.03125 to 0.03125
- bias_second: float32 [4], replicated, may hold values from -3 to 3
- w_latent: bfloat16 [2, 7168, 576], P(None, ('pd', 'seq')), may hold values from -0.0625 to 0.0625
- latent_gain: float32 [2, 512], replicated, may hold values from 0.5 to 1.5
- out_weight: bfloat16 [512, 7168], P(None, 'pd'), may hold values from -0.25 to 0.25
- span_slot: int32 [256], P('groups'), parts along dimension 0, may hold values from 0 to 63, each once
- block_owner: int32 [128], P('groups'), parts along dimension 0, may hold values from 0 to 31, each once
- prompt_length: int32 [4], P('groups'), parts along dimension 0, may hold values from 4096 to 8192
Outputs:
- cache: bfloat16 [2, 32768, 576], P(None, ('groups', 'seq')), parts along dimension 1
The draws below stay inside these ranges and needn't reach their ends.
There are 4 independent parts, one for each index of `groups`. The reference program is written for one: setup_inputs(seed, part) draws one part's arguments, and reference() takes and returns one part's arrays. A program takes and returns all parts, laid end to end along the dimension named above; an argument that names none is the same for every part. Nothing has to cross between parts.
Inputs may be any that keep to these rules, and one draw needn't show every extreme that they name: span_slot is a permutation; slot q lies in rows q * 128 to q * 128 + 127 of streams. block_owner is a permutation.
All inputs are finite; a program needn't handle non-finite values.
Results may differ from the reference program's by a relative error of at most 0.0058.
Values may be sent and summed in bfloat16 or wider, within the bound.
A program may use at most 128 MiB of HBM per device.

```python
import jax
import jax.numpy as jnp
from jax import lax

D = 7168
LAT = 512
ROPE = 64
KV = 576
RESIDUAL_WAYS = 4
SINK = 20
LAYERS = 2
TOK_DEV = 256
SPAN = 128
TOKENS = 8192
N_SEQ = 32


def block_scale(rng, extent, pieces, low, top_value):
    factor_of, own = 1.0, jax.random.fold_in(rng, 6)
    for dim, shards_of in pieces:
        heights = jnp.exp(jax.random.uniform(jax.random.fold_in(own, dim), (shards_of,), jnp.float32, low / len(pieces), top_value / len(pieces)))
        factor_of = factor_of * jnp.repeat(heights, extent[dim] // shards_of).reshape([-1 if axis == dim else 1 for axis in range(len(extent))])
    return factor_of


def centred(stream_key, extent, deviation, most, pieces=(), kind=jnp.bfloat16):
    factor_of = block_scale(stream_key, extent, pieces, -0.22, 0.18) if pieces else 1.0
    array = jax.random.normal(stream_key, extent, jnp.float32) * deviation * factor_of
    return jnp.minimum(jnp.maximum(array, -most), most).astype(kind)


def setup_inputs(seed: int = 0, part: int = 0) -> dict:
    streams_of = jax.random.split(jax.random.key(seed), 12)
    part_keys = jax.random.split(jax.random.fold_in(streams_of[11], part), 12)
    return {
        "streams": centred(part_keys[0], (TOKENS, RESIDUAL_WAYS, D), 1.0, 6.0, ((0, 32), (2, 2))),
        "mix_first": centred(streams_of[1], (RESIDUAL_WAYS, D, RESIDUAL_WAYS * RESIDUAL_WAYS + 2 * RESIDUAL_WAYS), (RESIDUAL_WAYS * D) ** -0.5, 0.03125, ((1, 2),)),
        "first_layer_bias": centred(streams_of[2], (RESIDUAL_WAYS * RESIDUAL_WAYS + 2 * RESIDUAL_WAYS,), 1.0, 3.0, (), jnp.float32),
        "pre_second": centred(streams_of[3], (RESIDUAL_WAYS, D, RESIDUAL_WAYS), (RESIDUAL_WAYS * D) ** -0.5, 0.03125, ((1, 2),)),
        "bias_second": centred(streams_of[4], (RESIDUAL_WAYS,), 1.0, 3.0, (), jnp.float32),
        "w_latent": centred(streams_of[5], (LAYERS, D, KV), D ** -0.5, 0.0625, ((1, 64),)),
        "latent_gain": jnp.clip(1.0 + 0.1 * jax.random.normal(streams_of[6], (LAYERS, LAT), jnp.float32), 0.5, 1.5),
        "out_weight": centred(streams_of[7], (LAT, D), LAT ** -0.5, 0.25, ((1, 2),)),
        "span_slot": jax.random.permutation(part_keys[8], 2 * N_SEQ).astype(jnp.int32),
        "block_owner": jax.random.permutation(part_keys[9], N_SEQ).astype(jnp.int32),
        "prompt_length": jax.random.randint(part_keys[10], (1,), TOKENS // 2, TOKENS + 1).astype(jnp.int32),
    }


EPSILON = 1e-06
THETA = 10000.0

def doubly_stochastic_normalize(blend_scores_raw):

    def one_sweep(turn_index, matrix):
        matrix = matrix / lax.optimization_barrier(jnp.sum(matrix, axis=2, keepdims=True))
        return matrix / lax.optimization_barrier(jnp.sum(matrix, axis=1, keepdims=True))
    return lax.fori_loop(0, SINK, one_sweep, jnp.exp(blend_scores_raw))

def combine(weights, stream_block):
    weighted = weights[:, 0, None] * stream_block[:, 0, :].astype(jnp.float32)
    for stream_index in range(1, RESIDUAL_WAYS):
        weighted = weighted + weights[:, stream_index, None] * stream_block[:, stream_index, :].astype(jnp.float32)
    return weighted

def coefficients(stream_block, weights, offsets):
    flattened = stream_block.reshape(stream_block.shape[0], -1)
    partial_value = jnp.dot(flattened, weights.reshape(flattened.shape[1], -1), preferred_element_type=jnp.float32)
    square_sum = lax.optimization_barrier(jnp.sum(jnp.square(flattened.astype(jnp.float32)), axis=1))
    rms_scale = jnp.sqrt(square_sum / flattened.shape[1] + EPSILON)
    return partial_value / rms_scale[:, None] + offsets[None, :]

def cache_entry(summed, places, gain_row):
    latent = summed[:, :LAT]
    mean_square = lax.optimization_barrier(jnp.mean(latent * latent, axis=1, keepdims=True))
    normed = latent * lax.rsqrt(mean_square + EPSILON) * gain_row[None, :]
    half_rope = ROPE // 2
    frequency = THETA ** (-jnp.arange(half_rope, dtype=jnp.float32) / half_rope)
    angles = places.astype(jnp.float32)[:, None] * frequency[None, :]
    first_half = summed[:, LAT:LAT + half_rope]
    second = summed[:, LAT + half_rope:]
    cosine_table = jnp.cos(angles)
    sine_values = jnp.sin(angles)
    rotated = jnp.concatenate([first_half * cosine_table - second * sine_values, second * cosine_table + first_half * sine_values], axis=1)
    return jnp.concatenate([normed, rotated], axis=1).astype(jnp.bfloat16)

def reference(streams, mix_first, first_layer_bias, pre_second, bias_second, w_latent, latent_gain, out_weight, span_slot, block_owner, prompt_length):
    total_rows = streams.shape[0]
    slot_span = jnp.zeros((2 * N_SEQ,), jnp.int32).at[span_slot].set(jnp.arange(2 * N_SEQ, dtype=jnp.int32))
    row_ids = jnp.arange(total_rows, dtype=jnp.int32)
    places = slot_span[row_ids // SPAN] * SPAN + row_ids % SPAN

    def one_block(payload):
        stream_block, block_places = payload
        blend_weight = coefficients(stream_block, mix_first, first_layer_bias)
        pre_gate = jax.nn.sigmoid(blend_weight[:, :RESIDUAL_WAYS])
        post_gate = 2.0 * jax.nn.sigmoid(blend_weight[:, RESIDUAL_WAYS:2 * RESIDUAL_WAYS])
        residual_blend_matrix = doubly_stochastic_normalize(blend_weight[:, 2 * RESIDUAL_WAYS:].reshape(-1, RESIDUAL_WAYS, RESIDUAL_WAYS))
        hidden = combine(pre_gate, stream_block).astype(jnp.bfloat16)
        entry_first = cache_entry(jnp.dot(hidden, w_latent[0], preferred_element_type=jnp.float32), block_places, latent_gain[0])
        branch = jnp.dot(entry_first[:, :LAT], out_weight, preferred_element_type=jnp.float32)
        updated = jnp.stack([combine(residual_blend_matrix[:, stream_index, :], stream_block) + post_gate[:, stream_index, None] * branch for stream_index in range(RESIDUAL_WAYS)], axis=1).astype(jnp.bfloat16)
        second_coef = coefficients(updated, pre_second, bias_second)
        hidden_second = combine(jax.nn.sigmoid(second_coef), updated).astype(jnp.bfloat16)
        entry_second = cache_entry(jnp.dot(hidden_second, w_latent[1], preferred_element_type=jnp.float32), block_places, latent_gain[1])
        return jnp.stack([entry_first, entry_second])
    blocks = streams.reshape(N_SEQ, TOK_DEV, RESIDUAL_WAYS, D)
    entries = lax.map(one_block, (blocks, places.reshape(N_SEQ, TOK_DEV)))
    entries = jnp.transpose(entries, (1, 0, 2, 3)).reshape(LAYERS, total_rows, KV)
    in_prompt = places < prompt_length[0]
    entries = jnp.where(in_prompt[None, :, None], entries, jnp.zeros((), jnp.bfloat16))
    row_of_place = jnp.zeros((total_rows,), jnp.int32).at[places].set(row_ids)
    home_segment_per_chip = jnp.zeros((N_SEQ,), jnp.int32).at[block_owner].set(jnp.arange(N_SEQ, dtype=jnp.int32))
    wanted = home_segment_per_chip[row_ids // TOK_DEV] * TOK_DEV + row_ids % TOK_DEV
    return entries[:, row_of_place[wanted], :]
```

```python
import functools
import math

import jax
import jax.numpy as jnp
import numpy as np
from jax import lax
from jax.experimental import pallas as pl
from jax.experimental.pallas import tpu as pltpu
from jax.sharding import PartitionSpec as P

LAT = 512
ROPE = 64
WAYS = 4
SINK = 20
EPSILON = 1e-06
THETA = 10000.0

LANES = 128
MESH = pl.DeviceIdType.MESH
BF16 = jnp.bfloat16
F32 = jnp.float32

FIRST = (0, 1, 2)
SECOND = (3, 4)
CROSS = {0: ("x", 5), 1: ("y", 6), 3: ("x", 7), 4: ("y", 8)}
ORDER = ((0, 1, 5, 6), (3, 4, 7, 8))


def kernel(
    n,
    ny,
    streams,
    mix,
    pre,
    w_in,
    out_w,
    bias1,
    bias2,
    gain,
    freq,
    slots,
    owners,
    length,
    out,
    raw,
    s4,
    wg,
    wl,
    mp,
    pp,
    hid,
    ow,
    cacc,
    cgot,
    ctr,
    cb,
    down,
    got,
    ent1,
    branch,
    trig,
    es,
    er,
    r1_first,
    r1_second,
    s2,
    r2,
    rp,
    rr1,
    rs2,
    rr2,
    rrp,
    ov,
    table,
    load_sem,
    zsend,
    zrecv,
    xsend,
    xrecv,
    psend,
    precv,
    asend,
    arecv,
    osem,
):
    me = lax.axis_index("seq")
    group = lax.axis_index("groups")
    core = lax.axis_index("pd")
    right = lax.rem(me + 1, n)
    left = lax.rem(me + n - 1, n)
    par_y = lax.rem(group, 2)
    par_x = lax.rem(lax.div(group, ny), 2)
    y_mate = group + 1 - 2 * par_y
    x_mate = group + (1 - 2 * par_x) * ny
    tokens, width = s4.shape[1:]
    r1 = (r1_first, r1_second)
    chunk = w_in.shape[1]
    span = tokens // 2
    cols = width // LANES
    entries = WAYS * width * 2

    barrier = pltpu.get_barrier_semaphore()
    for place in ({"seq": right}, {"seq": left}, {"groups": y_mate}, {"groups": x_mate}, {"pd": 1 - core}):
        pl.semaphore_signal(barrier, inc=1, device_id=place, device_id_type=MESH)

    def w_load():
        return pltpu.make_async_copy(w_in, wl, load_sem.at[0])

    def s_load(block):
        return pltpu.make_async_copy(
            streams.at[:, :, pl.ds(block * LANES, LANES)], raw.at[block], load_sem.at[1 + block]
        )

    def m_load(j):
        return pltpu.make_async_copy(mix.at[j], mp.at[pl.ds(j * 32, 24)], load_sem.at[1 + cols + j])

    def o_load():
        return pltpu.make_async_copy(out_w, ow, load_sem.at[5 + cols])

    w_load().start()
    for j in range(WAYS):
        m_load(j).start()
    for block in range(cols):
        s_load(block).start()
    o_load().start()

    own = pl.ds(pl.multiple_of(me * chunk, 16), chunk)
    w_load().wait()
    for layer in range(2):
        blocks = [wl[layer, :, b * LANES : (b + 1) * LANES] for b in range(4)]
        a_mine = jnp.where(par_x == 0, blocks[0], blocks[1])
        a_other = jnp.where(par_x == 0, blocks[1], blocks[0])
        b_mine = jnp.where(par_y == 0, blocks[2], blocks[3])
        b_other = jnp.where(par_y == 0, blocks[3], blocks[2])
        for slot, value in zip(ORDER[layer], (a_mine, b_mine, a_other, b_other)):
            wg[slot, own, :] = value
    wg[2, own, :] = jnp.concatenate([wl[0, :, LAT:], wl[1, :, LAT:]], axis=1)
    pl.semaphore_wait(barrier, 5)

    half = n // 2
    steps = (half, n - 1 - half)

    def z_copy(way, step, slot, source):
        rows = pl.ds(pl.multiple_of(source * chunk, 16), chunk)
        return pltpu.make_async_remote_copy(
            wg.at[slot, rows],
            wg.at[slot, rows],
            zsend.at[way, slot],
            zrecv.at[way, step - 1, slot],
            device_id={"seq": right if way == 0 else left},
            device_id_type=MESH,
        )

    def cross_copy(slot, source):
        axis, other = CROSS[slot]
        rows = pl.ds(pl.multiple_of(source * chunk, 16), chunk)
        return pltpu.make_async_remote_copy(
            wg.at[slot, rows],
            wg.at[other, rows],
            xsend.at[other - 5],
            xrecv.at[other - 5],
            device_id={"groups": x_mate if axis == "x" else y_mate},
            device_id_type=MESH,
        )

    def z_start(which):
        for slot in which:
            for way in (0, 1):
                z_copy(way, 1, slot, me).start()

    def z_step(which, step):
        for slot in which:
            for way in (0, 1):
                if step > steps[way]:
                    continue
                source = lax.rem(me + (n - step if way == 0 else step), n)
                z_copy(way, step, slot, source).wait_recv()
                if step < steps[way]:
                    z_copy(way, step + 1, slot, source).start()
                if slot in CROSS:
                    cross_copy(slot, source).start()

    def cross_whole(other):
        rows = wg.at[other, pl.ds(0, (n - 1) * chunk)]
        return pltpu.make_async_remote_copy(
            rows, rows, xsend.at[other - 5], xrecv.at[other - 5], device_id={"groups": x_mate}, device_id_type=MESH
        )

    def z_whole(way, slot):
        rows = wg.at[slot, pl.ds(0, steps[way] * chunk)]
        return pltpu.make_async_remote_copy(
            rows, rows, zsend.at[way, slot], zrecv.at[way, 0, slot], device_id={"seq": right}, device_id_type=MESH
        )

    def service(step):
        if step <= half:
            z_step(FIRST, step)
            z_step(SECOND, step)

    z_start(FIRST)
    z_start(SECOND)

    for j in range(WAYS):
        mp[j * 32 + 24 : j * 32 + 32, :] = jnp.zeros((8, width), BF16)
    row_id = lax.broadcasted_iota(jnp.int32, (256, 256), 0)
    col_id = lax.broadcasted_iota(jnp.int32, (256, 256), 1)
    sort = jnp.where(col_id == (row_id & 63) * 4 + (row_id >> 6), 1.0, 0.0).astype(BF16)
    lane_way = (
        lax.broadcasted_iota(jnp.int32, (256, LANES), 1) >> 5
        == lax.broadcasted_iota(jnp.int32, (256, LANES), 0) >> 6
    )
    cacc[...] = jnp.zeros_like(cacc)
    for j in range(WAYS):
        m_load(j).wait()

    def planes(q):
        for block in (2 * q, 2 * q + 1):
            s_load(block).wait()

        def body(part, carry):
            rows = pl.ds(pl.multiple_of(part * 64, 64), 64)
            pieces = [raw[block, pl.ds(part * 64, 64)].reshape(256, LANES) for block in (2 * q, 2 * q + 1)]
            sorted_rows = jnp.dot(sort, jnp.concatenate(pieces, axis=1), preferred_element_type=F32)
            narrow = sorted_rows.astype(BF16)
            for j in range(WAYS):
                s4[j, rows, q * 256 : q * 256 + 256] = narrow[j * 64 : j * 64 + 64]
            picked = lax.dot_general(
                narrow, mp[:, q * 256 : q * 256 + 256], (((1,), (1,)), ((), ())), preferred_element_type=F32
            )
            picked = jnp.where(lane_way, picked, 0.0)
            square = sorted_rows * sorted_rows
            square = square[:, :LANES] + square[:, LANES:]
            cacc[0, rows, :] += picked[:64] + picked[64:128] + picked[128:192] + picked[192:]
            cacc[1, rows, :] += square[:64] + square[64:128] + square[128:192] + square[192:]
            return carry

        lax.fori_loop(0, tokens // 64, body, 0)

    def pair_copy(source, target, index):
        return pltpu.make_async_remote_copy(
            source, target, psend.at[index], precv.at[index], device_id={"pd": 1 - core}, device_id_type=MESH
        )

    def own_span(which):
        slot = 2 * me + which
        return lax.fori_loop(
            0, 2 * n, lambda c, found: jnp.where(slots[c] == slot, c, found), jnp.int32(0)
        )

    spans_here = [own_span(0), own_span(1)]

    def trig_tables():
        for which in range(2):
            base = spans_here[which] * span
            place = (lax.broadcasted_iota(jnp.int32, (span, LANES), 0) + base).astype(F32)
            angle = place * freq[...]
            sign = jnp.where((lax.broadcasted_iota(jnp.int32, (span, LANES), 1) >> 5) & 1 == 0, -1.0, 1.0)
            trig[0, which * span : (which + 1) * span, :] = jnp.cos(angle)
            trig[1, which * span : (which + 1) * span, :] = jnp.sin(angle) * sign

    def wanted_table():
        def body(i, carry):
            block = jnp.int32(0)
            for b in range(n):
                block = jnp.where(owners[b] == i, b, block)
            table[2 * i] = slots[2 * block]
            table[2 * i + 1] = slots[2 * block + 1]
            return carry

        lax.fori_loop(0, n, body, 0)

    def first_gates():
        total = cacc[0] + cgot[0]
        total = total + pltpu.roll(total, 64, 1)
        total = total + pltpu.roll(total, 32, 1)
        square = jnp.sum(cacc[1] + cgot[1], axis=1, keepdims=True)
        scale = 1.0 / jnp.sqrt(square / entries + EPSILON)
        ctr[...] = jnp.transpose(total * scale + bias1[...])
        gates = jax.nn.sigmoid(ctr[0:8, :])
        doubled = lax.broadcasted_iota(jnp.int32, gates.shape, 0) >= WAYS
        gates = jnp.where(doubled, 2.0 * gates, gates)
        start = jnp.exp(ctr[8:24, :])
        matrix = tuple(start[k : k + 1, :] for k in range(WAYS * WAYS))

        def sweep(turn, m):
            m = list(m)
            for i in range(WAYS):
                inv = 1.0 / (m[4 * i] + m[4 * i + 1] + m[4 * i + 2] + m[4 * i + 3])
                for j in range(WAYS):
                    m[4 * i + j] = m[4 * i + j] * inv
            for j in range(WAYS):
                inv = 1.0 / (m[j] + m[4 + j] + m[8 + j] + m[12 + j])
                for i in range(WAYS):
                    m[4 * i + j] = m[4 * i + j] * inv
            return tuple(m)

        matrix = lax.fori_loop(0, SINK, sweep, matrix)
        ctr[0:8, :] = gates
        for k in range(WAYS * WAYS):
            ctr[8 + k : 9 + k, :] = matrix[k]

    def spread_gates():
        back = jnp.transpose(ctr[...])
        for k in range(24):
            cb[k] = jnp.broadcast_to(back[:, k : k + 1], (tokens, LANES))

    def combine_rows(lo, hi, first):
        def body(part, carry):
            rows = pl.ds(pl.multiple_of(part * 16, 16), 16)
            for tile in range(width // 512):
                c0 = tile * 512
                total = None
                for j in range(WAYS):
                    w = cb[first + j, rows, :]
                    term = jnp.concatenate([w] * 4, axis=1) * s4[j, rows, c0 : c0 + 512].astype(F32)
                    total = term if total is None else total + term
                hid[rows, c0 : c0 + 512] = total.astype(BF16)
            return carry

        lax.fori_loop(lo, hi, body, 0)

    def down_project(layer):
        slot_list = ORDER[layer] + (2,)

        def body(k, carry):
            k0 = pl.multiple_of(k * 512, 512)
            left_side = hid[:, pl.ds(k0, 512)]
            for c0, group_of in ((0, slot_list[0:2]), (256, slot_list[2:4]), (512, slot_list[4:5])):
                right_side = [wg[slot, pl.ds(k0, 512), :] for slot in group_of]
                right_side = right_side[0] if len(right_side) == 1 else jnp.concatenate(right_side, axis=1)
                part = jnp.dot(left_side, right_side, preferred_element_type=F32)
                wide = LANES * len(group_of)
                down[layer, :, c0 : c0 + wide] += part
            return carry

        down[layer] = jnp.zeros_like(down[layer])
        lax.fori_loop(0, width // 512, body, 0)

    def entry(layer):
        def body(part, carry):
            rows = pl.ds(pl.multiple_of(part * 32, 32), 32)
            summed = down[layer, rows, :] + got[layer, rows, :]
            latent = summed[:, :LAT]
            mean_square = jnp.sum(latent * latent, axis=1, keepdims=True) / LAT
            scale = lax.rsqrt(mean_square + EPSILON)
            m = [summed[:, b * LANES : (b + 1) * LANES] * scale for b in range(4)]
            blocks = [
                jnp.where(par_x == 0, m[0], m[2]),
                jnp.where(par_x == 0, m[2], m[0]),
                jnp.where(par_y == 0, m[1], m[3]),
                jnp.where(par_y == 0, m[3], m[1]),
            ]
            blocks = [blocks[b] * gain[layer : layer + 1, b * LANES : (b + 1) * LANES] for b in range(4)]
            which = lax.div(part, 4)
            base = jnp.where(which == 0, spans_here[0], spans_here[1]) * span + lax.rem(part, 4) * 32
            place = lax.broadcasted_iota(jnp.int32, (32, LANES), 0) + base
            inside = place < length[0]
            tile0 = pl.multiple_of(lax.rem(part, 4) * 4, 4)
            for h in range(2):
                block = jnp.where(core == 0, blocks[2 * h], blocks[2 * h + 1])
                es[layer, h, which, pl.ds(tile0, 4)] = (
                    jnp.where(inside, block, 0.0).reshape(4, 8, LANES).astype(BF16)
                )
            if layer == 0:
                ent1[rows, :] = jnp.concatenate(blocks, axis=1).astype(BF16)
            else:
                lane = lax.broadcasted_iota(jnp.int32, (32, LANES), 1)
                key = jnp.where(
                    lane < ROPE, down[0, rows, LAT:] + got[0, rows, LAT:], summed[:, LAT:]
                )
                swapped = jnp.where((lane >> 5) & 1 == 0, pltpu.roll(key, 96, 1), pltpu.roll(key, 32, 1))
                turned = key * trig[0, rows, :] + swapped * trig[1, rows, :]
                er[which, pl.ds(tile0, 4)] = jnp.where(inside, turned, 0.0).reshape(4, 8, LANES).astype(BF16)
            return carry

        lax.fori_loop(0, tokens // 32, body, 0)

    def update_tile(tile):
        c0 = tile * 512
        branch[...] = jnp.dot(ent1[...], ow[:, c0 : c0 + 512], preferred_element_type=F32)

        def body(part, carry):
            rows = pl.ds(pl.multiple_of(part * 16, 16), 16)
            for sub in range(4):
                d0 = c0 + sub * LANES
                old = [s4[j, rows, d0 : d0 + LANES].astype(F32) for j in range(WAYS)]
                add = branch[rows, sub * LANES : (sub + 1) * LANES]
                square = None
                for i in range(WAYS):
                    total = cb[WAYS + i, rows, :] * add
                    for j in range(WAYS):
                        total = total + cb[8 + 4 * i + j, rows, :] * old[j]
                    narrow = total.astype(BF16)
                    s4[i, rows, d0 : d0 + LANES] = narrow
                    wide = narrow.astype(F32)
                    square = wide * wide if square is None else square + wide * wide
                cacc[1, rows, :] += square
            return carry

        lax.fori_loop(0, tokens // 16, body, 0)
        total = None
        for j in range(WAYS):
            part = lax.dot_general(
                s4[j, :, c0 : c0 + 512],
                pp[j * 8 : j * 8 + 8, c0 : c0 + 512].astype(BF16),
                (((1,), (1,)), ((), ())),
                preferred_element_type=F32,
            )
            total = part if total is None else total + part
        cacc[0, :, 0:8] += total

    def second_gates():
        total = cacc[0] + cgot[2]
        square = jnp.sum(cacc[1] + cgot[3], axis=1, keepdims=True)
        scale = 1.0 / jnp.sqrt(square / entries + EPSILON)
        for k in range(WAYS):
            gate = jax.nn.sigmoid(total[:, k : k + 1] * scale + bias2[k])
            cb[k] = jnp.broadcast_to(gate, (tokens, LANES))

    def all_send(source_of, target, index):
        def body(d, carry):
            j = lax.rem(me + d, n)
            pltpu.make_async_remote_copy(
                source_of(j), target, asend.at[index], arecv.at[index], device_id={"seq": j}, device_id_type=MESH
            ).start()
            return carry

        lax.fori_loop(1, n, body, 0)

    def all_whole(buffer, index):
        rows = buffer.at[pl.ds(0, 2 * (n - 1))]
        return pltpu.make_async_remote_copy(
            rows, rows, asend.at[index], arecv.at[index], device_id={"seq": right}, device_id_type=MESH
        )

    def scatter_out(layer):
        all_send(
            lambda j: es.at[layer, lax.rem(j, 2), :, lax.div(j, 2)],
            r1[layer].at[pl.ds(2 * me, 2)],
            2 * layer,
        )
        r1[layer][pl.ds(2 * me, 2)] = es[layer, lax.rem(me, 2), :, lax.div(me, 2)]

    def forward_out(layer):
        all_whole(r1[layer], 2 * layer).wait_recv()

        def body(i, carry):
            s2[layer, 2 * i] = r1[layer][table[2 * i]]
            s2[layer, 2 * i + 1] = r1[layer][table[2 * i + 1]]
            return carry

        lax.fori_loop(0, n, body, 0)
        all_send(
            lambda j: s2.at[layer, pl.ds(2 * j, 2)],
            r2.at[layer, pl.ds(2 * me, 2)],
            2 * layer + 1,
        )
        r2[layer, pl.ds(2 * me, 2)] = s2[layer, pl.ds(2 * me, 2)]

    relays = n // 4
    relay = lax.rem(me, 4) == 3 * core
    relay_index = lax.div(me, 4)

    def key_part(count, index):
        rows = rr1.at[pl.ds(0, 2 * count)]
        return pltpu.make_async_remote_copy(
            rows, rows, asend.at[index], arecv.at[index], device_id={"seq": right}, device_id_type=MESH
        )

    def key_scatter():
        def body(m, carry):
            j = 4 * m + 3 * core
            r = 2 * m + core

            @pl.when(j != me)
            def _():
                pltpu.make_async_remote_copy(
                    er.at[:, r],
                    rr1.at[pl.ds(2 * me, 2)],
                    asend.at[4],
                    arecv.at[4],
                    device_id={"seq": j},
                    device_id_type=MESH,
                ).start()

            return carry

        lax.fori_loop(0, relays, body, 0)

        @pl.when(relay)
        def _():
            rr1[pl.ds(2 * me, 2)] = er[:, 2 * relay_index + core]

    def key_forward():
        @pl.when(relay)
        def _():
            key_part(n - 1, 4).wait_recv()

            def body(i, carry):
                rs2[2 * i] = rr1[table[2 * i]]
                rs2[2 * i + 1] = rr1[table[2 * i + 1]]
                return carry

            lax.fori_loop(0, n, body, 0)
            all_send(
                lambda j: rs2.at[pl.ds(2 * j, 2)],
                rr2.at[pl.ds(2 * relay_index, 2)],
                5,
            )
            rr2[pl.ds(2 * relay_index, 2)] = rs2[pl.ds(2 * me, 2)]

    def key_wait():
        @pl.when(relay)
        def _():
            key_part(relays - 1, 5).wait_recv()
            key_part(n - 1, 5).wait_send()
            key_part(relays - 1, 4).wait_send()

        @pl.when(jnp.logical_not(relay))
        def _():
            key_part(relays, 5).wait_recv()
            key_part(relays, 4).wait_send()

    def out_copy(layer):
        return pltpu.make_async_copy(ov.at[layer], out.at[layer], osem.at[layer])

    def arrange(layer):
        for h in range(2):
            for a in range(2):
                def tiles(ref):
                    rows = [ref[layer, 4 * r + 2 * h + a].astype(F32) for r in range(span // 8)]
                    return jnp.concatenate(rows, axis=0)

                mine, theirs = tiles(r2), tiles(rp)
                low = jnp.where(core == 0, mine, theirs).astype(BF16)
                high = jnp.where(core == 0, theirs, mine).astype(BF16)
                rows = slice(a * span, (a + 1) * span)
                ov[layer, rows, 2 * h * LANES : (2 * h + 1) * LANES] = low
                ov[layer, rows, (2 * h + 1) * LANES : (2 * h + 2) * LANES] = high

    def arrange_keys():
        for a in range(2):
            rows = []
            for r in range(span // 8):
                at = 2 * (r // 2) + a
                mine, theirs = rr2[at].astype(F32), rrp[at].astype(F32)
                rows.append(jnp.where(core == r % 2, mine, theirs))
            keys = jnp.concatenate(rows, axis=0).astype(BF16)
            where = slice(a * span, (a + 1) * span)
            ov[0, where, LAT:] = keys[:, :ROPE]
            ov[1, where, LAT:] = keys[:, ROPE:]

    work = [functools.partial(planes, q) for q in range(cols // 2)]
    step = 1
    for q in range(0, len(work), 2):
        for w in work[q : q + 2]:
            w()
        service(step)
        step += 1
    first_pair = pair_copy(cacc, cgot.at[pl.ds(0, 2)], 0)
    first_pair.start()
    trig_tables()
    service(step)
    step += 1
    first_pair.wait()
    first_gates()
    service(step)
    step += 1
    spread_gates()
    wanted_table()
    service(step)
    step += 1
    combine_rows(0, tokens // 32, 0)
    service(step)
    step += 1
    combine_rows(tokens // 32, tokens // 16, 0)
    service(step)
    step += 1
    cacc[...] = jnp.zeros_like(cacc)
    pp[...] = jnp.zeros_like(pp)
    for j in range(WAYS):
        pp[j * 8 : j * 8 + WAYS, :] = pre[j].astype(F32)
    while step <= half:
        service(step)
        step += 1
    cross_whole(5).wait_recv()
    cross_whole(6).wait_recv()

    down_project(0)
    pair_copy(down.at[0], got.at[0], 1).start()
    o_load().wait()
    pair_copy(down.at[0], got.at[0], 1).wait()
    entry(0)
    scatter_out(0)
    for tile in range(width // 512):
        update_tile(tile)
        if tile == 4:
            forward_out(0)
    second_pair = pair_copy(cacc, cgot.at[pl.ds(2, 2)], 2)
    second_pair.start()
    second_pair.wait()
    second_gates()
    combine_rows(0, tokens // 16, 0)
    cross_whole(7).wait_recv()
    cross_whole(8).wait_recv()
    down_project(1)
    pair_copy(down.at[1], got.at[1], 3).start()
    pair_copy(down.at[1], got.at[1], 3).wait()
    entry(1)
    key_scatter()
    scatter_out(1)
    all_whole(r2.at[0], 1).wait_recv()
    pair_copy(r2.at[0], rp.at[0], 4).start()
    pair_copy(r2.at[0], rp.at[0], 4).wait()
    arrange(0)
    key_forward()
    forward_out(1)
    for slot in FIRST + SECOND:
        for way in (0, 1):
            z_whole(way, slot).wait_send()
    for other in (5, 6, 7, 8):
        cross_whole(other).wait_send()
    for layer in range(2):
        all_whole(r1[layer], 2 * layer).wait_send()
    all_whole(r1[0], 1).wait_send()
    key_wait()
    pair_copy(rr2, rrp, 5).start()
    all_whole(r2.at[1], 3).wait_recv()
    pair_copy(r2.at[1], rp.at[1], 6).start()
    pair_copy(rr2, rrp, 5).wait()
    arrange_keys()
    out_copy(0).start()
    pair_copy(r2.at[1], rp.at[1], 6).wait()
    arrange(1)
    out_copy(1).start()
    all_whole(r1[1], 3).wait_send()
    out_copy(0).wait()
    out_copy(1).wait()


def solution(mesh):
    n = mesh.shape["seq"]
    groups = mesh.shape["groups"]
    ny = 2 ** math.ceil(math.log2(groups) / 2)

    def on_device(
        streams, mix_first, bias1, pre_second, bias2, w_latent, gain, out_weight, slots, owners, length
    ):
        tokens, ways, width = streams.shape
        chunk = w_latent.shape[1]
        cols = width // LANES
        full = n * chunk
        freq = THETA ** (-(np.arange(LANES) % (ROPE // 2)) / (ROPE // 2))
        vmem = pl.BlockSpec(memory_space=pltpu.VMEM)
        smem = pl.BlockSpec(memory_space=pltpu.SMEM)
        hbm = pl.BlockSpec(memory_space=pl.ANY)
        bias_row = jnp.pad(bias1[None, :], ((0, 0), (0, LANES - bias1.shape[0])))
        return pl.pallas_call(
            functools.partial(kernel, n, ny),
            out_shape=jax.ShapeDtypeStruct((2, tokens, LAT + ROPE), BF16),
            in_specs=[hbm, hbm, vmem, hbm, hbm, vmem, smem, vmem, vmem, smem, smem, smem],
            out_specs=hbm,
            scratch_shapes=[
                pltpu.VMEM((cols, tokens, ways, LANES), BF16),
                pltpu.VMEM((ways, tokens, width), BF16),
                pltpu.VMEM((9, full, LANES), BF16),
                pltpu.VMEM((2, chunk, LAT + ROPE), BF16),
                pltpu.VMEM((ways * 32, width), BF16),
                pltpu.VMEM((ways * 8, width), F32),
                pltpu.VMEM((tokens, width), BF16),
                pltpu.VMEM((LAT, width), BF16),
                pltpu.VMEM((2, tokens, LANES), F32),
                pltpu.VMEM((4, tokens, LANES), F32),
                pltpu.VMEM((LANES, tokens), F32),
                pltpu.VMEM((24, tokens, LANES), F32),
                pltpu.VMEM((2, tokens, LAT + LANES), F32),
                pltpu.VMEM((2, tokens, LAT + LANES), F32),
                pltpu.VMEM((tokens, LAT), BF16),
                pltpu.VMEM((tokens, 512), F32),
                pltpu.VMEM((2, tokens, LANES), F32),
                pltpu.VMEM((2, 2, 2, tokens // 16, 8, LANES), BF16),
                pltpu.VMEM((2, tokens // 16, 8, LANES), BF16),
                pltpu.VMEM((2 * n, 8, LANES), BF16),
                pltpu.VMEM((2 * n, 8, LANES), BF16),
                pltpu.VMEM((2, 2 * n, 8, LANES), BF16),
                pltpu.VMEM((2, 2 * n, 8, LANES), BF16),
                pltpu.VMEM((2, 2 * n, 8, LANES), BF16),
                pltpu.VMEM((2 * n, 8, LANES), BF16),
                pltpu.VMEM((2 * n, 8, LANES), BF16),
                pltpu.VMEM((n // 2, 8, LANES), BF16),
                pltpu.VMEM((n // 2, 8, LANES), BF16),
                pltpu.VMEM((2, tokens, LAT + ROPE), BF16),
                pltpu.SMEM((2 * n,), jnp.int32),
                pltpu.SemaphoreType.DMA((6 + cols,)),
                pltpu.SemaphoreType.DMA((2, 5)),
                pltpu.SemaphoreType.DMA((2, n // 2, 5)),
                pltpu.SemaphoreType.DMA((4,)),
                pltpu.SemaphoreType.DMA((4,)),
                pltpu.SemaphoreType.DMA((7,)),
                pltpu.SemaphoreType.DMA((7,)),
                pltpu.SemaphoreType.DMA((6,)),
                pltpu.SemaphoreType.DMA((6,)),
                pltpu.SemaphoreType.DMA((2,)),
            ],
            compiler_params=pltpu.CompilerParams(
                collective_id=0, has_side_effects=True, vmem_limit_bytes=61 * 2**20
            ),
        )(
            streams,
            jnp.transpose(mix_first, (0, 2, 1)),
            jnp.transpose(pre_second, (0, 2, 1)),
            w_latent,
            out_weight,
            bias_row,
            bias2,
            gain,
            jnp.asarray(freq[None, :], F32),
            slots,
            owners,
            length,
        )

    placed = (
        P(("groups", "seq"), None, "pd"),
        P(None, "pd", None),
        P(),
        P(None, "pd", None),
        P(),
        P(None, ("pd", "seq"), None),
        P(),
        P(None, "pd"),
        P("groups"),
        P("groups"),
        P("groups"),
    )
    return jax.shard_map(
        on_device, mesh=mesh, in_specs=placed, out_specs=P(None, ("groups", "seq"), None), check_vma=False
    )
```
